256 devices in a mesh: row: 32 (over z, y_lo, core), col: 8 (over y_hi, x).
Axes of the slice: x: 4, y: 4 (y_hi: 2, y_lo: 2; y = y_hi * 2 + y_lo), z: 8, core: 2. Of those that a mesh axis runs over, the one named last changes fastest.
Arguments:
- embeddings: bfloat16 [4096, 512], P('row'), may hold values from -16 to 16
- centers: bfloat16 [524288, 512], P(('row', 'col')), may hold values from -50 to 50
- labels: int32 [4096], replicated, may hold values from 0 to 524287
Outputs:
- loss: float32 [4096], P('row')
The draws below stay inside these ranges and needn't reach their ends.
All inputs are finite; a program needn't handle non-finite values.
Results may differ from the reference program's by a relative error of at most 0.00062.
Values may be sent and summed in bfloat16 or wider, within the bound.
No kernel may reach another device: no remote copies, remote signals or barrier semaphores. Data moves between devices by JAX's collectives and lax.ppermute only.
A program may use at most 64 MiB of HBM per device.

```python
import math
import jax
import jax.numpy as jnp
from jax import lax

D = 512
CLS_DEV = 2048
TOKENS = 4096
CLASSES = 524288


def label_draw(key):
    return jax.random.randint(jax.random.fold_in(key, 17), (TOKENS,), 0, CLASSES, dtype=jnp.int32)


def class_vectors(key, row_tag, share, class_ids):
    basis = jnp.clip(jax.random.normal(jax.random.fold_in(key, 11), (16, D), jnp.float32), -4.0, 4.0)
    row_key = jax.random.fold_in(key, row_tag)

    def one_class(index):
        own_key = jax.random.fold_in(row_key, index)
        factors = jnp.clip(jax.random.normal(jax.random.fold_in(own_key, 0), (16,), jnp.float32), -4.0, 4.0)
        noise = jnp.clip(jax.random.normal(jax.random.fold_in(own_key, 1), (D,), jnp.float32), -4.0, 4.0)
        return (factors, noise)
    factors, noise = jax.vmap(one_class)(class_ids)
    shared = jnp.dot(factors, basis, precision=lax.Precision.HIGHEST) * 0.25
    return math.sqrt(share) * shared + math.sqrt(1.0 - share) * noise


def unit_float(values):
    return values / jnp.sqrt(jnp.sum(values * values, axis=1, keepdims=True) + 1e-06)


def draw_labels(key, part):
    return label_draw(key)


def draw_centers(key, part):
    share = 0.35
    values = class_vectors(key, 13, share, jnp.arange(CLASSES, dtype=jnp.int32))
    return values.astype(jnp.bfloat16)


def draw_embeddings(key, part):
    share = 0.35
    cos_low = 0.5
    cos_high = 0.95
    mix_low = 0.2
    mix_high = 0.7
    scale_high = 3.0
    close_mix = 0.995
    labels = label_draw(key)
    rivals = jax.random.randint(jax.random.fold_in(key, 29), (TOKENS,), 0, CLASSES, dtype=jnp.int32)
    target_dir = unit_float(class_vectors(key, 13, share, labels))
    rival_dir = unit_float(class_vectors(key, 13, share, rivals))
    rest = class_vectors(key, 31, share, jnp.arange(TOKENS, dtype=jnp.int32))
    rest = rest - jnp.sum(rest * target_dir, axis=1, keepdims=True) * target_dir
    rest = rest - jnp.sum(rest * rival_dir, axis=1, keepdims=True) * rival_dir
    rest = unit_float(rest)
    target_cos = jax.random.uniform(jax.random.fold_in(key, 37), (TOKENS, 1), jnp.float32, cos_low, cos_high)
    mix = jax.random.uniform(jax.random.fold_in(key, 41), (TOKENS, 1), jnp.float32, mix_low, mix_high)
    close_rows = jax.random.randint(jax.random.fold_in(key, 47), (TOKENS, 1), 0, 8, dtype=jnp.int32) == 0
    close_cos = jax.random.uniform(jax.random.fold_in(key, 53), (TOKENS, 1), jnp.float32, 0.05, 0.2)
    target_cos = jnp.where(close_rows, close_cos, target_cos)
    mix = jnp.where(close_rows, close_mix, mix)
    side = jnp.sqrt(1.0 - target_cos * target_cos)
    values = target_cos * target_dir + side * mix * rival_dir + side * jnp.sqrt(1.0 - mix * mix) * rest
    row_scale = jnp.exp(jax.random.uniform(jax.random.fold_in(key, 43), (TOKENS, 1), jnp.float32, math.log(2.0), math.log(scale_high)))
    return (values * row_scale).astype(jnp.bfloat16)


def setup_inputs(seed: int = 0) -> dict:
    arg_keys = jax.random.split(jax.random.key(seed), 4)
    return {
        "embeddings": draw_embeddings(jax.random.fold_in(arg_keys[3], 71), 0),
        "centers": draw_centers(jax.random.fold_in(arg_keys[3], 71), 0),
        "labels": draw_labels(jax.random.fold_in(arg_keys[3], 71), 0),
    }


logit_scale = 128.0
margin_angle = 0.5

def unit_rows(values):
    values = values.astype(jnp.float32)
    length = jnp.sqrt(lax.optimization_barrier(jnp.sum(values * values, axis=1, keepdims=True)))
    return (values / jnp.maximum(length, 1.0)).astype(jnp.bfloat16)

def margin_cos(cosine):
    sine = jnp.sqrt(jnp.maximum(1.0 - cosine * cosine, 0.0))
    return cosine * math.cos(margin_angle) - sine * math.sin(margin_angle)

def block_stats(emb_unit, row_labels, center_unit, first_class):
    cosine = lax.dot_general(emb_unit, center_unit, (((1,), (1,)), ((), ())), preferred_element_type=jnp.float32)
    class_ids = first_class + lax.iota(jnp.int32, center_unit.shape[0])
    target = row_labels[:, None] == class_ids[None, :]
    scores = logit_scale * jnp.where(target, margin_cos(cosine), cosine)
    peak = lax.optimization_barrier(jnp.max(scores, axis=1))
    total = lax.optimization_barrier(jnp.sum(jnp.exp(scores - peak[:, None]), axis=1))
    target_cos = lax.optimization_barrier(jnp.sum(jnp.where(target, cosine, 0.0), axis=1))
    return (peak, total, target_cos)

def fold_stats(state, fresh):
    peak = jnp.maximum(state[0], fresh[0])
    total = state[1] * jnp.exp(state[0] - peak) + fresh[1] * jnp.exp(fresh[0] - peak)
    return (peak, total, state[2] + fresh[2])

def reference(embeddings, centers, labels):
    emb_unit = unit_rows(embeddings)
    blocks = CLASSES // CLS_DEV
    center_blocks = centers.reshape(blocks, CLS_DEV, D)
    start = (jnp.full((TOKENS,), -2.0 * logit_scale, jnp.float32), jnp.zeros((TOKENS,), jnp.float32), jnp.zeros((TOKENS,), jnp.float32))

    def advance(state, inputs):
        block, index = inputs
        fresh = block_stats(emb_unit, labels, unit_rows(block), (index * CLS_DEV).astype(jnp.int32))
        return (fold_stats(state, fresh), None)
    state, _ = lax.scan(advance, start, (center_blocks, jnp.arange(blocks, dtype=jnp.int32)))
    peak, total, target_cos = state
    return peak + jnp.log(total) - logit_scale * margin_cos(target_cos)
```

```python
import functools
import math

import jax
import jax.numpy as jnp
from jax import lax
from jax.experimental import pallas as pl
from jax.experimental.pallas import tpu as pltpu
from jax.sharding import Mesh
from jax.sharding import PartitionSpec as P


AXES = ("z", "yl", "co", "yh", "x")
ROW = ("z", "yl", "co")
SAME_CORE = ("z", "yl", "yh", "x")

f32 = jnp.float32
bf16 = jnp.bfloat16
logit_scale = 128.0
margin_angle = 0.5
SCALE2 = logit_scale * math.log2(math.e)
NEVER = -4.0
CHUNK = 256


def unit_rows(values):
    values = values.astype(f32)
    length = jnp.sqrt(jnp.sum(values * values, axis=1, keepdims=True))
    return (values / jnp.maximum(length, 1.0)).astype(bf16)


def margin_cos(cosine):
    sine = jnp.sqrt(jnp.maximum(1.0 - cosine * cosine, 0.0))
    return cosine * math.cos(margin_angle) - sine * math.sin(margin_angle)


def unit_kernel(*refs):
    out_ref = refs[-1]
    at = 0
    for ref in refs[:-1]:
        rows = ref.shape[0]
        step = min(rows, 256)

        def one(i, _, ref=ref, step=step, at=at):
            out_ref[pl.ds(at + i * step, step), :] = unit_rows(ref[pl.ds(i * step, step), :])
            return 0

        lax.fori_loop(0, rows // step, one, 0)
        at += rows


def unit_call(*parts):
    rows, width = sum(p.shape[0] for p in parts), parts[0].shape[1]
    return pl.pallas_call(
        unit_kernel,
        out_shape=jax.ShapeDtypeStruct((rows, width), bf16),
        in_specs=[pl.BlockSpec(memory_space=pltpu.VMEM)] * len(parts),
        out_specs=pl.BlockSpec(memory_space=pltpu.VMEM),
        compiler_params=pltpu.CompilerParams(vmem_limit_bytes=16 * 2**20),
        cost_estimate=pl.CostEstimate(
            flops=rows * 2**19, bytes_accessed=rows * width * 4, transcendentals=rows
        ),
        name=f"unit{rows}",
    )(*parts)


def block_of(step, flip):
    depth = lax.axis_size("z")
    z = lax.rem(lax.axis_index("z") + step % depth, depth)
    yl = lax.axis_index("yl")
    return z, (1 - yl if flip else yl)


def first_class(core, half):
    z, yl = lax.axis_index("z"), lax.axis_index("yl")
    col = lax.axis_index("yh") * lax.axis_size("x") + lax.axis_index("x")
    cols = lax.axis_size("yh") * lax.axis_size("x")
    return (((z * 2 + yl) * 2 + core) * cols + col) * half


def stats_kernel(steps, lab_ref, *refs):
    count = len(steps)
    e_refs, (own_ref, other_ref, out_ref, e_all, s_own, s_other) = refs[:count], refs[count:]
    rows = e_all.shape[0]
    blocks, half = rows // 128, own_ref.shape[0]
    at = 0
    for ref in e_refs:
        e_all[at : at + ref.shape[0], :] = ref[...]
        at += ref.shape[0]
    wanted = []
    co = lax.axis_index("co")
    own_first, other_first = first_class(co, half), first_class(1 - co, half)
    for b in range(blocks):
        z, yl = block_of(steps[b // 2], b % 2)
        line = lab_ref[pl.ds(z * 4 + yl * 2 + co, 1), :]
        own, other = line - own_first, line - other_first
        in_own = (own >= 0) & (own < half)
        in_other = (other >= 0) & (other < half)
        wanted.append(jnp.where(in_own, own, jnp.where(in_other, other + half, -100)))
    wanted = jnp.concatenate(wanted, axis=1) if blocks > 1 else wanted[0]
    place = jnp.broadcast_to(wanted, (8, rows)) - lax.broadcasted_iota(jnp.int32, (8, rows), 0)

    def product(index, c_ref, s_ref):
        s_ref[...] = lax.dot_general(
            c_ref[pl.ds(index * CHUNK, CHUNK), :],
            e_all[...],
            (((1,), (1,)), ((), ())),
            preferred_element_type=f32,
        )

    def fold(first, s_ref, state):
        peak, total, found = state
        tops = [None] * 4
        for j in range(CHUNK // 8):
            cosine = s_ref[j * 8 : (j + 1) * 8, :]
            hit = place == (first + j * 8)
            found = jnp.where(hit, cosine, found)
            cosine = jnp.where(hit, NEVER, cosine)
            s_ref[j * 8 : (j + 1) * 8, :] = cosine
            k = j % 4
            tops[k] = cosine if tops[k] is None else jnp.maximum(tops[k], cosine)
        fresh = jnp.maximum(peak, functools.reduce(jnp.maximum, tops))
        sums = [total * jnp.exp2((peak - fresh) * SCALE2)] + [None] * 3
        for j in range(CHUNK // 8):
            term = jnp.exp2((s_ref[j * 8 : (j + 1) * 8, :] - fresh) * SCALE2)
            k = j % 4
            sums[k] = term if sums[k] is None else sums[k] + term
        return fresh, functools.reduce(jnp.add, sums), found

    product(0, own_ref, s_own)

    def body(k, state):
        product(k, other_ref, s_other)
        state = fold(k * CHUNK, s_own, state)
        product(jnp.minimum(k + 1, half // CHUNK - 1), own_ref, s_own)
        return fold(half + k * CHUNK, s_other, state)

    peak, total, found = lax.fori_loop(
        0,
        half // CHUNK,
        body,
        (
            jnp.full((8, rows), NEVER, f32),
            jnp.zeros((8, rows), f32),
            jnp.full((8, rows), 2 * NEVER, f32),
        ),
    )
    found = jnp.max(found, axis=0, keepdims=True)
    here = found > NEVER
    margin = margin_cos(found)
    top = jnp.max(peak, axis=0, keepdims=True)
    top = jnp.where(here, jnp.maximum(top, margin), top)
    total = jnp.sum(total * jnp.exp2((peak - top) * SCALE2), axis=0, keepdims=True)
    total = total + jnp.where(here, jnp.exp2((margin - top) * SCALE2), 0.0)
    log_total = logit_scale * top + jnp.log(total)
    target = jnp.where(here, logit_scale * margin, 0.0)
    for b in range(blocks):
        part = slice(b * 128, (b + 1) * 128)
        out_ref[b, :, 0:128] = log_total[:, part]
        out_ref[b, :, 128:256] = target[:, part]


def stats_call(parts, own, other, labels, steps):
    rows = sum(p.shape[0] for p in parts)
    width = own.shape[1]
    classes = own.shape[0] + other.shape[0]
    return pl.pallas_call(
        functools.partial(stats_kernel, tuple(steps)),
        out_shape=jax.ShapeDtypeStruct((rows // 128, 1, 256), f32),
        in_specs=[pl.BlockSpec(memory_space=pltpu.VMEM)] * (3 + len(parts)),
        out_specs=pl.BlockSpec(memory_space=pltpu.VMEM),
        scratch_shapes=[
            pltpu.VMEM((rows, width), bf16),
            pltpu.VMEM((CHUNK, rows), f32),
            pltpu.VMEM((CHUNK, rows), f32),
        ],
        compiler_params=pltpu.CompilerParams(vmem_limit_bytes=20 * 2**20),
        cost_estimate=pl.CostEstimate(
            flops=2 * rows * classes * width,
            bytes_accessed=classes * width * 2,
            transcendentals=rows * classes,
        ),
        name=f"stats{rows}",
    )(labels, *parts, own, other)


def spread_kernel(steps, copies, *refs):
    out_ref = refs[-1]
    order = iter(steps)
    for ref in refs[:-1]:
        for b in range(ref.shape[0]):
            if b % 2 == 0:
                step = next(order)
            z, yl = block_of(step, b % 2)
            place = pl.multiple_of((z * 2 + yl) * copies, copies)
            out_ref[pl.ds(place, copies)] = jnp.broadcast_to(ref[b : b + 1], (copies, 1, 256))


def spread_call(found, steps, copies):
    total = sum(f.shape[0] for f in found)
    return pl.pallas_call(
        functools.partial(spread_kernel, tuple(steps), copies),
        out_shape=jax.ShapeDtypeStruct((total * copies, 1, 256), f32),
        in_specs=[pl.BlockSpec(memory_space=pltpu.VMEM)] * len(found),
        out_specs=pl.BlockSpec(memory_space=pltpu.VMEM),
        name="spread",
    )(*found)


def moved(value, axis, by):
    n = lax.axis_size(axis)
    return lax.ppermute(value, axis, [(i, (i + by) % n) for i in range(n)])


def shards(embeddings, centers, labels):
    depth = lax.axis_size("z")
    cols = lax.axis_size("yh") * lax.axis_size("x")
    other_raw = moved(centers, "co", 1)
    neighbour = moved(embeddings, "yl", 1)
    own = unit_call(centers)
    own, neighbour = lax.optimization_barrier((own, neighbour))
    mine = unit_call(embeddings, neighbour)
    other = unit_call(other_raw)
    lines = labels.reshape(-1, 128)
    results, order = [], []

    def visit(parts, steps):
        results.append(stats_call(parts, own, other, lines, steps))
        order.extend(steps)

    up, down = mine, mine
    waiting = ([mine], [0])
    for step in range(1, (depth + 1) // 2):
        up, down = moved(up, "z", 1), moved(down, "z", -1)
        visit(*waiting)
        up, down, results[-1] = lax.optimization_barrier((up, down, results[-1]))
        waiting = ([up, down], [-step, step])
    if depth % 2 == 0:
        up = moved(up, "z", 1)
        visit(*waiting)
        up, results[-1] = lax.optimization_barrier((up, results[-1]))
        waiting = ([up], [-(depth // 2)])
    visit(*waiting)

    sent = spread_call(results, order, cols)
    got = lax.all_to_all(sent, SAME_CORE, split_axis=0, concat_axis=0, tiled=True)
    got = got.reshape(-1, 2, 128)
    log_total, target = got[:, 0], got[:, 1]
    peak = jnp.max(log_total, axis=0)
    total = jnp.sum(jnp.exp(log_total - peak), axis=0)
    return peak + jnp.log(total) - jnp.sum(target, axis=0)


def solution(mesh):
    split = Mesh(mesh.devices.reshape(8, 2, 2, 2, 4), AXES)
    return jax.shard_map(
        shards,
        mesh=split,
        in_specs=(P(ROW, None), P(AXES, None), P()),
        out_specs=P(ROW),
        check_vma=False,
    )
```

```python
import functools
import math

import jax
import jax.numpy as jnp
from jax import lax
from jax.experimental import pallas as pl
from jax.experimental.pallas import tpu as pltpu
from jax.sharding import Mesh
from jax.sharding import PartitionSpec as P


AXES = ("z", "yl", "co", "yh", "x")
ROW = ("z", "yl", "co")
SAME_CORE = ("z", "yl", "yh", "x")

f32 = jnp.float32
bf16 = jnp.bfloat16
logit_scale = 128.0
margin_angle = 0.5
SCALE2 = logit_scale * math.log2(math.e)
NEVER = -4.0
SHIFT = 80.0
UNROLL = 4


def unit_rows(values):
    values = values.astype(f32)
    length = jnp.sqrt(jnp.sum(values * values, axis=1, keepdims=True))
    return (values / jnp.maximum(length, 1.0)).astype(bf16)


def margin_cos(cosine):
    sine = jnp.sqrt(jnp.maximum(1.0 - cosine * cosine, 0.0))
    return cosine * math.cos(margin_angle) - sine * math.sin(margin_angle)


def unit_kernel(*refs):
    at = 0
    for ref in refs[:-1]:
        refs[-1][at : at + ref.shape[0], :] = unit_rows(ref[...])
        at += ref.shape[0]


def unit_call(*parts):
    rows, width = sum(p.shape[0] for p in parts), parts[0].shape[1]
    tile = 256 if len(parts) == 1 else rows
    specs = [pl.BlockSpec((min(tile, p.shape[0]), width), lambda i: (i, 0)) for p in parts]
    return pl.pallas_call(
        unit_kernel,
        grid=(rows // tile,),
        out_shape=jax.ShapeDtypeStruct((rows, width), bf16),
        in_specs=specs,
        out_specs=pl.BlockSpec((tile, width), lambda i: (i, 0)),
        compiler_params=pltpu.CompilerParams(vmem_limit_bytes=8 * 2**20),
        cost_estimate=pl.CostEstimate(
            flops=rows * 2**19, bytes_accessed=rows * width * 4, transcendentals=rows
        ),
        name=f"unit{rows}",
    )(*parts)


def block_of(step, flip):
    depth = lax.axis_size("z")
    z = lax.rem(lax.axis_index("z") + step % depth, depth)
    yl = lax.axis_index("yl")
    return z, (1 - yl if flip else yl)


def first_class(core, half):
    z, yl = lax.axis_index("z"), lax.axis_index("yl")
    col = lax.axis_index("yh") * lax.axis_size("x") + lax.axis_index("x")
    cols = lax.axis_size("yh") * lax.axis_size("x")
    return (((z * 2 + yl) * 2 + core) * cols + col) * half


def stats_kernel(places, chunk, lab_ref, own_ref, other_ref, *refs):
    count = len(places)
    e_refs, (out_ref, e_all, s_own, s_other) = refs[:count], refs[-4:]
    rows, half = e_all.shape[0], own_ref.shape[0]
    co = lax.axis_index("co")
    own_first, other_first = first_class(co, half), first_class(1 - co, half)
    wanted, blocks, at = [], [], 0
    for ref, steps in zip(e_refs, places):
        e_all[at : at + ref.shape[0], :] = ref[...]
        at += ref.shape[0]
        for step, flip in steps:
            z, yl = block_of(step, flip)
            line = lab_ref[pl.ds(z * 4 + yl * 2 + co, 1), :]
            own, other = line - own_first, line - other_first
            in_own = (own >= 0) & (own < half)
            in_other = (other >= 0) & (other < half)
            wanted.append(jnp.where(in_own, own, jnp.where(in_other, other + half, -100)))
            blocks.append(z * 2 + yl)
    wanted = jnp.concatenate(wanted, axis=1) if len(wanted) > 1 else wanted[0]
    place = jnp.broadcast_to(wanted, (8, rows)) - lax.broadcasted_iota(jnp.int32, (8, rows), 0)
    turns = half // chunk

    def product(index, c_ref, s_ref):
        s_ref[...] = lax.dot_general(
            c_ref[pl.ds(index * chunk, chunk), :],
            e_all[...],
            (((1,), (1,)), ((), ())),
            preferred_element_type=f32,
        )

    def finish(total, found, shift):
        found = jnp.max(found, axis=0, keepdims=True)
        here = found > NEVER
        margin = margin_cos(found)
        if shift is None:
            peak, total = total
            top = jnp.max(peak, axis=0, keepdims=True)
            top = jnp.where(here, jnp.maximum(top, margin), top)
            total, shift = total * jnp.exp2((peak - top) * SCALE2), top * SCALE2
        total = jnp.sum(total, axis=0, keepdims=True)
        both = total + jnp.where(here, jnp.exp2(margin * SCALE2 - shift), 0.0)
        log_total = (jnp.log2(both) + shift) * math.log(2.0)
        target = jnp.where(here, logit_scale * margin, 0.0)
        copies = out_ref.shape[0] // 16
        for b, block in enumerate(blocks):
            part = slice(b * 128, (b + 1) * 128)
            line = jnp.concatenate([log_total[:, part], target[:, part]], axis=1)
            spot = pl.multiple_of(block * copies, copies)
            out_ref[pl.ds(spot, copies)] = jnp.broadcast_to(line[None], (copies, 1, 256))
        return total

    def fold(first, s_ref, state):
        sums, found = list(state[:-1]), state[-1]
        here = place - first
        for j in range(chunk // 8):
            cosine = s_ref[j * 8 : (j + 1) * 8, :]
            hit = here == j * 8
            found = jnp.where(hit, cosine, found)
            term = jnp.exp2(jnp.where(hit, NEVER, cosine) * SCALE2 - SHIFT)
            sums[j % len(sums)] = sums[j % len(sums)] + term
        return (*sums, found)

    product(0, own_ref, s_own)

    def body(k, state):
        for turn in range(UNROLL):
            t = k * UNROLL + turn
            product(t, other_ref, s_other)
            state = fold(t * chunk, s_own, state)
            product(jnp.minimum(t + 1, turns - 1), own_ref, s_own)
            state = fold(half + t * chunk, s_other, state)
        return state

    zero, none = jnp.zeros((8, rows), f32), jnp.full((8, rows), 2 * NEVER, f32)
    state = lax.fori_loop(0, turns // UNROLL, body, (zero,) * (1024 // rows) + (none,))
    total = finish(functools.reduce(jnp.add, state[:-1]), state[-1], SHIFT)

    @pl.when(jnp.min(total) < 2.0**-89)
    def _():
        def careful(first, s_ref, state):
            def one(j, state):
                peak, total, found = state
                cosine = s_ref[pl.ds(pl.multiple_of(j * 8, 8), 8), :]
                hit = place == first + j * 8
                found = jnp.where(hit, cosine, found)
                cosine = jnp.where(hit, NEVER, cosine)
                top = jnp.maximum(peak, cosine)
                total = total * jnp.exp2((peak - top) * SCALE2) + jnp.exp2((cosine - top) * SCALE2)
                return top, total, found

            return lax.fori_loop(0, chunk // 8, one, state)

        def again(k, state):
            product(k, own_ref, s_own)
            state = careful(k * chunk, s_own, state)
            product(k, other_ref, s_other)
            return careful(half + k * chunk, s_other, state)

        peak, total, found = lax.fori_loop(0, turns, again, (none * 0.5, zero, none))
        finish((peak, total), found, None)


def stats_call(board, parts, places, own, other, labels):
    rows, width = sum(p.shape[0] for p in parts), own.shape[1]
    classes = own.shape[0] + other.shape[0]
    shape = (16 * lax.axis_size("yh") * lax.axis_size("x"), 1, 256)
    chunk = 256
    boards = () if board is None else (board,)
    return pl.pallas_call(
        functools.partial(stats_kernel, tuple(places), chunk),
        out_shape=jax.ShapeDtypeStruct(shape, f32),
        in_specs=[pl.BlockSpec(memory_space=pltpu.VMEM)] * (3 + len(parts))
        + [pl.BlockSpec(memory_space=pltpu.VMEM)] * len(boards),
        out_specs=pl.BlockSpec(memory_space=pltpu.VMEM),
        scratch_shapes=[
            pltpu.VMEM((rows, width), bf16),
            pltpu.VMEM((chunk, rows), f32),
            pltpu.VMEM((chunk, rows), f32),
        ],
        input_output_aliases={3 + len(parts): 0} if boards else {},
        compiler_params=pltpu.CompilerParams(vmem_limit_bytes=16 * 2**20),
        cost_estimate=pl.CostEstimate(
            flops=2 * rows * classes * width,
            bytes_accessed=classes * width * 2,
            transcendentals=rows * classes,
        ),
        name=f"stats{rows}",
    )(labels, own, other, *parts, *boards)


def moved(value, axis, by):
    n = lax.axis_size(axis)
    return lax.ppermute(value, axis, [(i, (i + by) % n) for i in range(n)])


def to_lower(value):
    spots = [(yl, yh) for yl in range(2) for yh in range(2)]
    pairs = []
    for yl, yh in spots:
        y = (yh * 2 + yl + (1 if yl else -1)) % 4
        pairs.append((spots.index((yl, yh)), spots.index((y % 2, y // 2))))
    return lax.ppermute(value, ("yl", "yh"), pairs)


def shards(embeddings, centers, labels):
    fence = lax.optimization_barrier
    up1, down1 = moved(embeddings, "z", 1), moved(embeddings, "z", -1)
    beside = moved(embeddings, "yl", 1)
    other = moved(centers, "co", 1)
    lines = labels.reshape(-1, 128)
    own = unit_call(centers)

    up1, down1, own = fence((up1, down1, own))
    up2, down2 = moved(up1, "z", 1), moved(down1, "z", -1)
    pair1 = unit_call(up1, down1)
    side1 = moved(pair1, "yl", 1)
    mine = unit_call(embeddings, beside)
    other = unit_call(other)
    board = stats_call(None, [mine], [[(0, 0), (0, 1)]], own, other, lines)

    up2, down2, board = fence((up2, down2, board))
    up3, down3 = moved(up2, "z", 1), moved(down2, "z", -1)
    pair2 = unit_call(up2, down2)
    side2 = moved(pair2, "yl", 1)
    board = stats_call(
        board, [pair1, side1], [[(-1, 0), (1, 0)], [(-1, 1), (1, 1)]], own, other, lines
    )

    up3, down3, board = fence((up3, down3, board))
    far = moved(up3, "z", 1)
    pair3 = unit_call(up3, down3)
    side3 = to_lower(pair3)
    board = stats_call(
        board, [pair2, side2], [[(-2, 0), (2, 0)], [(-2, 1), (2, 1)]], own, other, lines
    )

    far, board = fence((far, board))
    far_side = moved(far, "yl", 1)
    board = stats_call(board, [pair3], [[(-3, 0), (3, 0)]], own, other, lines)
    side3, far_side, board = fence((side3, far_side, board))
    opposite = unit_call(far, far_side)
    board = stats_call(
        board, [side3, opposite], [[(-3, 1), (3, 1)], [(4, 0), (4, 1)]], own, other, lines
    )

    got = lax.all_to_all(board, SAME_CORE, split_axis=0, concat_axis=0, tiled=True)
    got = got.reshape(-1, 2, 128)
    log_total, target = got[:, 0], got[:, 1]
    peak = jnp.max(log_total, axis=0)
    total = jnp.sum(jnp.exp(log_total - peak), axis=0)
    return peak + jnp.log(total) - jnp.sum(target, axis=0)


def solution(mesh):
    split = Mesh(mesh.devices.reshape(8, 2, 2, 2, 4), AXES)
    return jax.shard_map(
        shards,
        mesh=split,
        in_specs=(P(ROW, None), P(AXES, None), P()),
        out_specs=P(ROW),
        check_vma=False,
    )
```

```python
import functools
import math

import jax
import jax.numpy as jnp
from jax import lax
from jax.experimental import pallas as pl
from jax.experimental.pallas import tpu as pltpu
from jax.sharding import Mesh
from jax.sharding import PartitionSpec as P


AXES = ("z", "yl", "co", "yh", "x")
ROW = ("z", "yl", "co")
SAME_CORE = ("z", "yl", "yh", "x")

f32 = jnp.float32
bf16 = jnp.bfloat16
logit_scale = 128.0
margin_angle = 0.5
SCALE2 = logit_scale * math.log2(math.e)
NEVER = -4.0
SHIFT = 80.0
UNROLL = 8


def unit_rows(values):
    values = values.astype(f32)
    length = jnp.sqrt(jnp.sum(values * values, axis=1, keepdims=True))
    return (values / jnp.maximum(length, 1.0)).astype(bf16)


def margin_cos(cosine):
    sine = jnp.sqrt(jnp.maximum(1.0 - cosine * cosine, 0.0))
    return cosine * math.cos(margin_angle) - sine * math.sin(margin_angle)


def unit_kernel(*refs):
    at = 0
    for ref in refs[:-1]:
        refs[-1][at : at + ref.shape[0], :] = unit_rows(ref[...])
        at += ref.shape[0]


def unit_call(*parts):
    rows, width = sum(p.shape[0] for p in parts), parts[0].shape[1]
    return pl.pallas_call(
        unit_kernel,
        out_shape=jax.ShapeDtypeStruct((rows, width), bf16),
        in_specs=[pl.BlockSpec(memory_space=pltpu.VMEM)] * len(parts),
        out_specs=pl.BlockSpec(memory_space=pltpu.VMEM),
        compiler_params=pltpu.CompilerParams(vmem_limit_bytes=8 * 2**20),
        cost_estimate=pl.CostEstimate(
            flops=rows * 2**19, bytes_accessed=rows * width * 4, transcendentals=rows
        ),
    )(*parts)


def centers_kernel(raw_ref, out_ref, held, sems):
    pieces = sems.shape[0]
    rows = out_ref.shape[0] // pieces
    copies = [
        pltpu.make_async_copy(
            raw_ref.at[pl.ds(i * rows, rows)], held.at[pl.ds(i * rows, rows)], sems.at[i]
        )
        for i in range(pieces)
    ]
    for copy in copies:
        copy.start()
    for i, copy in enumerate(copies):
        copy.wait()
        out_ref[i * rows : (i + 1) * rows, :] = unit_rows(held[i * rows : (i + 1) * rows, :])


def unit_centers(centers, pieces=8):
    return pl.pallas_call(
        centers_kernel,
        out_shape=jax.ShapeDtypeStruct(centers.shape, bf16),
        in_specs=[pl.BlockSpec(memory_space=pltpu.MemorySpace.HBM)],
        out_specs=pl.BlockSpec(memory_space=pltpu.VMEM),
        scratch_shapes=[pltpu.VMEM(centers.shape, bf16), pltpu.SemaphoreType.DMA((pieces,))],
        compiler_params=pltpu.CompilerParams(vmem_limit_bytes=50 * 2**20),
        cost_estimate=pl.CostEstimate(
            flops=centers.shape[0] * 2**19,
            bytes_accessed=centers.size * 4,
            transcendentals=centers.shape[0],
        ),
        name="centers",
    )(centers)


def block_of(step, flip):
    depth = lax.axis_size("z")
    z = lax.rem(lax.axis_index("z") + step % depth, depth)
    yl = lax.axis_index("yl")
    return z, (1 - yl if flip else yl)


def first_class(core, half):
    z, yl = lax.axis_index("z"), lax.axis_index("yl")
    col = lax.axis_index("yh") * lax.axis_size("x") + lax.axis_index("x")
    cols = lax.axis_size("yh") * lax.axis_size("x")
    return (((z * 2 + yl) * 2 + core) * cols + col) * half


def stats_kernel(places, chunk, lab_ref, own_ref, other_ref, *refs):
    count = len(places)
    e_refs, (out_ref, e_all, s_own, s_other) = refs[:count], refs[-4:]
    rows, half = e_all.shape[0], own_ref.shape[0]
    co = lax.axis_index("co")
    own_first, other_first = first_class(co, half), first_class(1 - co, half)
    wanted, blocks, at = [], [], 0
    for ref, steps in zip(e_refs, places):
        e_all[at : at + ref.shape[0], :] = ref[...]
        at += ref.shape[0]
        for step, flip in steps:
            z, yl = block_of(step, flip)
            line = lab_ref[pl.ds(z * 4 + yl * 2 + co, 1), :]
            own, other = line - own_first, line - other_first
            in_own = (own >= 0) & (own < half)
            in_other = (other >= 0) & (other < half)
            wanted.append(jnp.where(in_own, own, jnp.where(in_other, other + half, -100)))
            blocks.append(z * 2 + yl)
    wanted = jnp.concatenate(wanted, axis=1) if len(wanted) > 1 else wanted[0]
    place = jnp.broadcast_to(wanted, (8, rows)) - lax.broadcasted_iota(jnp.int32, (8, rows), 0)
    turns = half // chunk

    def product(index, c_ref, s_ref):
        s_ref[...] = lax.dot_general(
            c_ref[pl.ds(index * chunk, chunk), :],
            e_all[...],
            (((1,), (1,)), ((), ())),
            preferred_element_type=f32,
        )

    def finish(total, found, shift):
        found = jnp.max(found, axis=0, keepdims=True)
        here = found > NEVER
        margin = margin_cos(found)
        if shift is None:
            peak, total = total
            top = jnp.max(peak, axis=0, keepdims=True)
            top = jnp.where(here, jnp.maximum(top, margin), top)
            total, shift = total * jnp.exp2((peak - top) * SCALE2), top * SCALE2
        total = jnp.sum(total, axis=0, keepdims=True)
        both = total + jnp.where(here, jnp.exp2(margin * SCALE2 - shift), 0.0)
        log_total = (jnp.log2(both) + shift) * math.log(2.0)
        target = jnp.where(here, logit_scale * margin, 0.0)
        copies = out_ref.shape[0] // 16
        for b, block in enumerate(blocks):
            part = slice(b * 128, (b + 1) * 128)
            line = jnp.concatenate([log_total[:, part], target[:, part]], axis=1)
            spot = pl.multiple_of(block * copies, copies)
            out_ref[pl.ds(spot, copies)] = jnp.broadcast_to(line[None], (copies, 1, 256))
        return total

    def fold(first, s_ref, state):
        sums, found = list(state[:-1]), state[-1]
        here = place - first
        for j in range(chunk // 8):
            cosine = s_ref[j * 8 : (j + 1) * 8, :]
            hit = here == j * 8
            found = jnp.where(hit, cosine, found)
            term = jnp.exp2(jnp.where(hit, NEVER, cosine) * SCALE2 - SHIFT)
            sums[j % len(sums)] = sums[j % len(sums)] + term
        return (*sums, found)

    product(0, own_ref, s_own)

    def body(k, state):
        for turn in range(UNROLL):
            t = k * UNROLL + turn
            product(t, other_ref, s_other)
            state = fold(t * chunk, s_own, state)
            product(jnp.minimum(t + 1, turns - 1), own_ref, s_own)
            state = fold(half + t * chunk, s_other, state)
        return state

    zero, none = jnp.zeros((8, rows), f32), jnp.full((8, rows), 2 * NEVER, f32)
    state = lax.fori_loop(0, turns // UNROLL, body, (zero,) * (1024 // rows) + (none,))
    total = finish(functools.reduce(jnp.add, state[:-1]), state[-1], SHIFT)

    @pl.when(jnp.min(total) < 2.0**-89)
    def _():
        def careful(first, s_ref, state):
            def one(j, state):
                peak, total, found = state
                cosine = s_ref[pl.ds(pl.multiple_of(j * 8, 8), 8), :]
                hit = place == first + j * 8
                found = jnp.where(hit, cosine, found)
                cosine = jnp.where(hit, NEVER, cosine)
                top = jnp.maximum(peak, cosine)
                total = total * jnp.exp2((peak - top) * SCALE2) + jnp.exp2((cosine - top) * SCALE2)
                return top, total, found

            return lax.fori_loop(0, chunk // 8, one, state)

        def again(k, state):
            product(k, own_ref, s_own)
            state = careful(k * chunk, s_own, state)
            product(k, other_ref, s_other)
            return careful(half + k * chunk, s_other, state)

        peak, total, found = lax.fori_loop(0, turns, again, (none * 0.5, zero, none))
        finish((peak, total), found, None)


def stats_call(board, parts, places, own, other, labels):
    rows, width = sum(p.shape[0] for p in parts), own.shape[1]
    classes = own.shape[0] + other.shape[0]
    shape = (16 * lax.axis_size("yh") * lax.axis_size("x"), 1, 256)
    chunk = 256
    boards = () if board is None else (board,)
    return pl.pallas_call(
        functools.partial(stats_kernel, tuple(places), chunk),
        out_shape=jax.ShapeDtypeStruct(shape, f32),
        in_specs=[pl.BlockSpec(memory_space=pltpu.VMEM)] * (3 + len(parts))
        + [pl.BlockSpec(memory_space=pltpu.VMEM)] * len(boards),
        out_specs=pl.BlockSpec(memory_space=pltpu.VMEM),
        scratch_shapes=[
            pltpu.VMEM((rows, width), bf16),
            pltpu.VMEM((chunk, rows), f32),
            pltpu.VMEM((chunk, rows), f32),
        ],
        input_output_aliases={3 + len(parts): 0} if boards else {},
        compiler_params=pltpu.CompilerParams(vmem_limit_bytes=16 * 2**20),
        cost_estimate=pl.CostEstimate(
            flops=2 * rows * classes * width,
            bytes_accessed=classes * width * 2,
            transcendentals=rows * classes,
        ),
    )(labels, own, other, *parts, *boards)


def moved(value, axis, by):
    n = lax.axis_size(axis)
    return lax.ppermute(value, axis, [(i, (i + by) % n) for i in range(n)])


def to_lower(value):
    spots = [(yl, yh) for yl in range(2) for yh in range(2)]
    pairs = []
    for yl, yh in spots:
        y = (yh * 2 + yl + (1 if yl else -1)) % 4
        pairs.append((spots.index((yl, yh)), spots.index((y % 2, y // 2))))
    return lax.ppermute(value, ("yl", "yh"), pairs)


def crossed(value):
    depth = lax.axis_size("z")
    pairs = [(z * 2 + yl, (z - 1) % depth * 2 + 1 - yl) for z in range(depth) for yl in range(2)]
    return lax.ppermute(value, ("z", "yl"), pairs)


def shards(embeddings, centers, labels):
    fence = lax.optimization_barrier
    up1 = moved(embeddings, "z", 1)
    down1 = moved(embeddings, "z", -1)
    beside = moved(embeddings, "yl", 1)
    lines = labels.reshape(-1, 128)
    own = unit_centers(centers)
    other = moved(own, "co", 1)

    up1, down1, own = fence((up1, down1, own))
    up2 = moved(up1, "z", 1)
    down2 = moved(down1, "z", -1)
    pair1 = unit_call(up1, down1)
    side1 = moved(pair1, "yl", 1)
    mine = unit_call(embeddings, beside)
    board = stats_call(None, [mine], [[(0, 0), (0, 1)]], own, other, lines)

    up2, down2, board = fence((up2, down2, board))
    up3 = moved(up2, "z", 1)
    down3 = moved(down2, "z", -1)
    pair2 = unit_call(up2, down2)
    side2 = moved(pair2, "yl", 1)
    board = stats_call(
        board, [pair1, side1], [[(-1, 0), (1, 0)], [(-1, 1), (1, 1)]], own, other, lines
    )

    up3, down3, board = fence((up3, down3, board))
    pair3 = unit_call(up3, down3)
    side3 = to_lower(pair3)
    far, far_side = moved(up3, "z", 1), crossed(down3)
    board = stats_call(
        board, [pair2, pair3], [[(-2, 0), (2, 0)], [(-3, 0), (3, 0)]], own, other, lines
    )
    far, far_side, side2, board = fence((far, far_side, side2, board))
    opposite = unit_call(far, far_side)
    board = stats_call(
        board, [side2, opposite], [[(-2, 1), (2, 1)], [(4, 0), (4, 1)]], own, other, lines
    )
    side3, board = fence((side3, board))
    board = stats_call(board, [side3], [[(-3, 1), (3, 1)]], own, other, lines)

    got = lax.all_to_all(board, SAME_CORE, split_axis=0, concat_axis=0, tiled=True)
    got = got.reshape(-1, 2, 128)
    log_total, target = got[:, 0], got[:, 1]
    peak = jnp.max(log_total, axis=0)
    total = jnp.sum(jnp.exp(log_total - peak), axis=0)
    return peak + jnp.log(total) - jnp.sum(target, axis=0)


def solution(mesh):
    split = Mesh(mesh.devices.reshape(8, 2, 2, 2, 4), AXES)
    return jax.shard_map(
        shards,
        mesh=split,
        in_specs=(P(ROW, None), P(AXES, None), P()),
        out_specs=P(ROW),
        check_vma=False,
    )
```

```python
import functools
import math

import jax
import jax.numpy as jnp
from jax import lax
from jax.experimental import pallas as pl
from jax.experimental.pallas import tpu as pltpu
from jax.sharding import Mesh
from jax.sharding import PartitionSpec as P


AXES = ("z", "yl", "co", "yh", "x")
ROW = ("z", "yl", "co")
SAME_CORE = ("z", "yl", "yh", "x")

f32 = jnp.float32
bf16 = jnp.bfloat16
logit_scale = 128.0
margin_angle = 0.5
SCALE2 = logit_scale * math.log2(math.e)
NEVER = -4.0
SHIFT = 80.0
UNROLL = 8


def unit_rows(values):
    values = values.astype(f32)
    length = jnp.sqrt(jnp.sum(values * values, axis=1, keepdims=True))
    return (values / jnp.maximum(length, 1.0)).astype(bf16)


def margin_cos(cosine):
    sine = jnp.sqrt(jnp.maximum(1.0 - cosine * cosine, 0.0))
    return cosine * math.cos(margin_angle) - sine * math.sin(margin_angle)


def unit_kernel(*refs):
    at = 0
    for ref in refs[:-1]:
        refs[-1][at : at + ref.shape[0], :] = unit_rows(ref[...])
        at += ref.shape[0]


def unit_call(*parts):
    rows, width = sum(p.shape[0] for p in parts), parts[0].shape[1]
    return pl.pallas_call(
        unit_kernel,
        out_shape=jax.ShapeDtypeStruct((rows, width), bf16),
        in_specs=[pl.BlockSpec(memory_space=pltpu.VMEM)] * len(parts),
        out_specs=pl.BlockSpec(memory_space=pltpu.VMEM),
        compiler_params=pltpu.CompilerParams(vmem_limit_bytes=8 * 2**20),
        cost_estimate=pl.CostEstimate(
            flops=rows * 2**19, bytes_accessed=rows * width * 4, transcendentals=rows
        ),
    )(*parts)


def centers_kernel(raw_ref, out_ref, held, sems):
    pieces = sems.shape[0]
    rows = out_ref.shape[0] // pieces
    copies = [
        pltpu.make_async_copy(
            raw_ref.at[pl.ds(i * rows, rows)], held.at[pl.ds(i * rows, rows)], sems.at[i]
        )
        for i in range(pieces)
    ]
    for copy in copies:
        copy.start()
    for i, copy in enumerate(copies):
        copy.wait()
        out_ref[i * rows : (i + 1) * rows, :] = unit_rows(held[i * rows : (i + 1) * rows, :])


def unit_centers(centers, pieces=8):
    return pl.pallas_call(
        centers_kernel,
        out_shape=jax.ShapeDtypeStruct(centers.shape, bf16),
        in_specs=[pl.BlockSpec(memory_space=pltpu.MemorySpace.HBM)],
        out_specs=pl.BlockSpec(memory_space=pltpu.VMEM),
        scratch_shapes=[pltpu.VMEM(centers.shape, bf16), pltpu.SemaphoreType.DMA((pieces,))],
        compiler_params=pltpu.CompilerParams(vmem_limit_bytes=50 * 2**20),
        cost_estimate=pl.CostEstimate(
            flops=centers.shape[0] * 2**19,
            bytes_accessed=centers.size * 4,
            transcendentals=centers.shape[0],
        ),
        name="centers",
    )(centers)


def block_of(step, flip):
    depth = lax.axis_size("z")
    z = lax.rem(lax.axis_index("z") + step % depth, depth)
    yl = lax.axis_index("yl")
    return z, (1 - yl if flip else yl)


def first_class(core, half):
    z, yl = lax.axis_index("z"), lax.axis_index("yl")
    col = lax.axis_index("yh") * lax.axis_size("x") + lax.axis_index("x")
    cols = lax.axis_size("yh") * lax.axis_size("x")
    return (((z * 2 + yl) * 2 + core) * cols + col) * half


def stats_kernel(places, raw, chunk, lab_ref, own_ref, other_ref, *refs):
    count = len(places)
    e_refs, (out_ref, e_all, s_own, s_other) = refs[:count], refs[-4:]
    rows, half = e_all.shape[0], own_ref.shape[0]
    co = lax.axis_index("co")
    own_first, other_first = first_class(co, half), first_class(1 - co, half)
    wanted, blocks, at = [], [], 0
    for ref, steps in zip(e_refs, places):
        e_all[at : at + ref.shape[0], :] = unit_rows(ref[...]) if raw else ref[...]
        at += ref.shape[0]
        for step, flip in steps:
            z, yl = block_of(step, flip)
            line = lab_ref[pl.ds(z * 4 + yl * 2 + co, 1), :]
            own, other = line - own_first, line - other_first
            in_own = (own >= 0) & (own < half)
            in_other = (other >= 0) & (other < half)
            wanted.append(jnp.where(in_own, own, jnp.where(in_other, other + half, -100)))
            blocks.append(z * 2 + yl)
    wanted = jnp.concatenate(wanted, axis=1) if len(wanted) > 1 else wanted[0]
    place = jnp.broadcast_to(wanted, (8, rows)) - lax.broadcasted_iota(jnp.int32, (8, rows), 0)
    turns = half // chunk

    def product(index, c_ref, s_ref):
        s_ref[...] = lax.dot_general(
            c_ref[pl.ds(index * chunk, chunk), :],
            e_all[...],
            (((1,), (1,)), ((), ())),
            preferred_element_type=f32,
        )

    def finish(total, found, shift):
        found = jnp.max(found, axis=0, keepdims=True)
        here = found > NEVER
        margin = margin_cos(found)
        if shift is None:
            peak, total = total
            top = jnp.max(peak, axis=0, keepdims=True)
            top = jnp.where(here, jnp.maximum(top, margin), top)
            total, shift = total * jnp.exp2((peak - top) * SCALE2), top * SCALE2
        total = jnp.sum(total, axis=0, keepdims=True)
        both = total + jnp.where(here, jnp.exp2(margin * SCALE2 - shift), 0.0)
        log_total = (jnp.log2(both) + shift) * math.log(2.0)
        target = jnp.where(here, logit_scale * margin, 0.0)
        copies = out_ref.shape[0] // 16
        for b, block in enumerate(blocks):
            part = slice(b * 128, (b + 1) * 128)
            line = jnp.concatenate([log_total[:, part], target[:, part]], axis=1)
            spot = pl.multiple_of(block * copies, copies)
            out_ref[pl.ds(spot, copies)] = jnp.broadcast_to(line[None], (copies, 1, 256))
        return total

    def fold(first, s_ref, state):
        sums, found = list(state[:-1]), state[-1]
        here = place - first
        for j in range(chunk // 8):
            cosine = s_ref[j * 8 : (j + 1) * 8, :]
            hit = here == j * 8
            found = jnp.where(hit, cosine, found)
            term = jnp.exp2(jnp.where(hit, NEVER, cosine) * SCALE2 - SHIFT)
            sums[j % len(sums)] = sums[j % len(sums)] + term
        return (*sums, found)

    product(0, own_ref, s_own)

    def body(k, state):
        for turn in range(UNROLL):
            t = k * UNROLL + turn
            product(t, other_ref, s_other)
            state = fold(t * chunk, s_own, state)
            product(jnp.minimum(t + 1, turns - 1), own_ref, s_own)
            state = fold(half + t * chunk, s_other, state)
        return state

    zero, none = jnp.zeros((8, rows), f32), jnp.full((8, rows), 2 * NEVER, f32)
    state = lax.fori_loop(0, turns // UNROLL, body, (zero,) * (1024 // rows) + (none,))
    total = finish(functools.reduce(jnp.add, state[:-1]), state[-1], SHIFT)

    @pl.when(jnp.min(total) < 2.0**-89)
    def _():
        def careful(first, s_ref, state):
            def one(j, state):
                peak, total, found = state
                cosine = s_ref[pl.ds(pl.multiple_of(j * 8, 8), 8), :]
                hit = place == first + j * 8
                found = jnp.where(hit, cosine, found)
                cosine = jnp.where(hit, NEVER, cosine)
                top = jnp.maximum(peak, cosine)
                total = total * jnp.exp2((peak - top) * SCALE2) + jnp.exp2((cosine - top) * SCALE2)
                return top, total, found

            return lax.fori_loop(0, chunk // 8, one, state)

        def again(k, state):
            product(k, own_ref, s_own)
            state = careful(k * chunk, s_own, state)
            product(k, other_ref, s_other)
            return careful(half + k * chunk, s_other, state)

        peak, total, found = lax.fori_loop(0, turns, again, (none * 0.5, zero, none))
        finish((peak, total), found, None)


def stats_call(board, parts, places, own, other, labels, raw=False):
    rows, width = sum(p.shape[0] for p in parts), own.shape[1]
    classes = own.shape[0] + other.shape[0]
    shape = (16 * lax.axis_size("yh") * lax.axis_size("x"), 1, 256)
    chunk = 256
    boards = () if board is None else (board,)
    return pl.pallas_call(
        functools.partial(stats_kernel, tuple(places), raw, chunk),
        out_shape=jax.ShapeDtypeStruct(shape, f32),
        in_specs=[pl.BlockSpec(memory_space=pltpu.VMEM)] * (3 + len(parts))
        + [pl.BlockSpec(memory_space=pltpu.VMEM)] * len(boards),
        out_specs=pl.BlockSpec(memory_space=pltpu.VMEM),
        scratch_shapes=[
            pltpu.VMEM((rows, width), bf16),
            pltpu.VMEM((chunk, rows), f32),
            pltpu.VMEM((chunk, rows), f32),
        ],
        input_output_aliases={3 + len(parts): 0} if boards else {},
        compiler_params=pltpu.CompilerParams(vmem_limit_bytes=16 * 2**20),
        cost_estimate=pl.CostEstimate(
            flops=2 * rows * classes * width,
            bytes_accessed=classes * width * 2,
            transcendentals=rows * classes,
        ),
    )(labels, own, other, *parts, *boards)


def combine_kernel(got_ref, out_ref):
    n = got_ref.shape[0] // 8
    even = lax.rem(lax.broadcasted_iota(jnp.int32, (8, 128), 0), 2) == 0
    tiles = [got_ref[i * 8 : (i + 1) * 8, :] for i in range(n)]
    peak = functools.reduce(jnp.maximum, tiles)
    peak = jnp.max(jnp.where(even, peak, -2.0 * logit_scale), axis=0, keepdims=True)
    sums = [jnp.zeros((8, 128), f32)] * 4
    for i, tile in enumerate(tiles):
        fall = jnp.where(even, (tile - peak) * math.log2(math.e), -1000.0)
        sums[i % 4] = sums[i % 4] + jnp.exp2(fall)
    total = jnp.sum(functools.reduce(jnp.add, sums), axis=0, keepdims=True)
    target = functools.reduce(jnp.add, tiles)
    target = jnp.sum(jnp.where(even, 0.0, target), axis=0, keepdims=True)
    out_ref[...] = peak + jnp.log(total) - target


def combine_call(got):
    return pl.pallas_call(
        combine_kernel,
        out_shape=jax.ShapeDtypeStruct((1, 128), f32),
        in_specs=[pl.BlockSpec(memory_space=pltpu.VMEM)],
        out_specs=pl.BlockSpec(memory_space=pltpu.VMEM),
        compiler_params=pltpu.CompilerParams(vmem_limit_bytes=2**20),
        name="combine",
    )(got)


def moved(value, axis, by):
    n = lax.axis_size(axis)
    return lax.ppermute(value, axis, [(i, (i + by) % n) for i in range(n)])


def to_lower(value):
    spots = [(yl, yh) for yl in range(2) for yh in range(2)]
    pairs = []
    for yl, yh in spots:
        y = (yh * 2 + yl + (1 if yl else -1)) % 4
        pairs.append((spots.index((yl, yh)), spots.index((y % 2, y // 2))))
    return lax.ppermute(value, ("yl", "yh"), pairs)


def shards(embeddings, centers, labels):
    fence = lax.optimization_barrier
    up1 = moved(embeddings, "z", 1)
    down1 = moved(embeddings, "z", -1)
    beside = moved(embeddings, "yl", 1)
    lines = labels.reshape(-1, 128)
    own = unit_centers(centers)
    other = moved(own, "co", 1)

    up1, down1, own = fence((up1, down1, own))
    up2 = moved(up1, "z", 1)
    down2 = moved(down1, "z", -1)
    pair1 = unit_call(up1, down1)
    side1 = moved(pair1, "yl", 1)
    board = stats_call(
        None, [embeddings, beside], [[(0, 0)], [(0, 1)]], own, other, lines, raw=True
    )

    up2, down2, board = fence((up2, down2, board))
    up3 = moved(up2, "z", 1)
    down3 = moved(down2, "z", -1)
    pair2 = unit_call(up2, down2)
    side2 = moved(pair2, "yl", 1)
    board = stats_call(
        board, [pair1, side1], [[(-1, 0), (1, 0)], [(-1, 1), (1, 1)]], own, other, lines
    )

    up3, down3, board = fence((up3, down3, board))
    far = moved(up3, "z", 1)
    pair3 = unit_call(up3, down3)
    side3 = to_lower(pair3)
    board = stats_call(
        board, [pair2, pair3], [[(-2, 0), (2, 0)], [(-3, 0), (3, 0)]], own, other, lines
    )
    far, board = fence((far, board))
    far_side = moved(far, "yl", 1)
    side2, board = fence((side2, board))
    board = stats_call(board, [side2], [[(-2, 1), (2, 1)]], own, other, lines)
    side3, board = fence((side3, board))
    board = stats_call(board, [side3], [[(-3, 1), (3, 1)]], own, other, lines)
    far_side, board = fence((far_side, board))
    board = stats_call(board, [far, far_side], [[(4, 0)], [(4, 1)]], own, other, lines, raw=True)

    got = lax.all_to_all(board, SAME_CORE, split_axis=0, concat_axis=0, tiled=True)
    return combine_call(got.reshape(-1, 128)).reshape(-1)


def solution(mesh):
    split = Mesh(mesh.devices.reshape(8, 2, 2, 2, 4), AXES)
    return jax.shard_map(
        shards,
        mesh=split,
        in_specs=(P(ROW, None), P(AXES, None), P()),
        out_specs=P(ROW),
        check_vma=False,
    )
```

```python
import functools
import math

import jax
import jax.numpy as jnp
from jax import lax
from jax.experimental import pallas as pl
from jax.experimental.pallas import tpu as pltpu
from jax.sharding import Mesh
from jax.sharding import PartitionSpec as P


AXES = ("z", "yl", "co", "yh", "x")
ROW = ("z", "yl", "co")
SAME_CORE = ("z", "yl", "yh", "x")

f32 = jnp.float32
bf16 = jnp.bfloat16
logit_scale = 128.0
margin_angle = 0.5
SCALE2 = logit_scale * math.log2(math.e)
NEVER = -4.0
SHIFT = 80.0
UNROLL = 8


def unit_rows(values):
    values = values.astype(f32)
    length = jnp.sqrt(jnp.sum(values * values, axis=1, keepdims=True))
    return (values / jnp.maximum(length, 1.0)).astype(bf16)


def margin_cos(cosine):
    sine = jnp.sqrt(jnp.maximum(1.0 - cosine * cosine, 0.0))
    return cosine * math.cos(margin_angle) - sine * math.sin(margin_angle)


def unit_kernel(*refs):
    at = 0
    for ref in refs[:-1]:
        refs[-1][at : at + ref.shape[0], :] = unit_rows(ref[...])
        at += ref.shape[0]


def unit_call(*parts):
    rows, width = sum(p.shape[0] for p in parts), parts[0].shape[1]
    return pl.pallas_call(
        unit_kernel,
        out_shape=jax.ShapeDtypeStruct((rows, width), bf16),
        in_specs=[pl.BlockSpec(memory_space=pltpu.VMEM)] * len(parts),
        out_specs=pl.BlockSpec(memory_space=pltpu.VMEM),
        compiler_params=pltpu.CompilerParams(vmem_limit_bytes=8 * 2**20),
        cost_estimate=pl.CostEstimate(
            flops=rows * 2**19, bytes_accessed=rows * width * 4, transcendentals=rows
        ),
    )(*parts)


def centers_kernel(raw_ref, out_ref, held, sems):
    pieces = sems.shape[0]
    rows = out_ref.shape[0] // pieces
    copies = [
        pltpu.make_async_copy(
            raw_ref.at[pl.ds(i * rows, rows)], held.at[pl.ds(i * rows, rows)], sems.at[i]
        )
        for i in range(pieces)
    ]
    for copy in copies:
        copy.start()
    for i, copy in enumerate(copies):
        copy.wait()
        out_ref[i * rows : (i + 1) * rows, :] = unit_rows(held[i * rows : (i + 1) * rows, :])


def unit_centers(centers, pieces=8):
    return pl.pallas_call(
        centers_kernel,
        out_shape=jax.ShapeDtypeStruct(centers.shape, bf16),
        in_specs=[pl.BlockSpec(memory_space=pltpu.MemorySpace.HBM)],
        out_specs=pl.BlockSpec(memory_space=pltpu.VMEM),
        scratch_shapes=[pltpu.VMEM(centers.shape, bf16), pltpu.SemaphoreType.DMA((pieces,))],
        compiler_params=pltpu.CompilerParams(vmem_limit_bytes=50 * 2**20),
        cost_estimate=pl.CostEstimate(
            flops=centers.shape[0] * 2**19,
            bytes_accessed=centers.size * 4,
            transcendentals=centers.shape[0],
        ),
        name="centers",
    )(centers)


def block_of(step, flip):
    depth = lax.axis_size("z")
    z = lax.rem(lax.axis_index("z") + step % depth, depth)
    yl = lax.axis_index("yl")
    return z, (1 - yl if flip else yl)


def first_class(core, half):
    z, yl = lax.axis_index("z"), lax.axis_index("yl")
    col = lax.axis_index("yh") * lax.axis_size("x") + lax.axis_index("x")
    cols = lax.axis_size("yh") * lax.axis_size("x")
    return (((z * 2 + yl) * 2 + core) * cols + col) * half


def stats_kernel(places, raw, chunk, lab_ref, own_ref, other_ref, *refs):
    count = len(places)
    e_refs, (out_ref, e_all, s_own, s_other) = refs[:count], refs[-4:]
    rows, half = e_all.shape[0], own_ref.shape[0]
    co = lax.axis_index("co")
    own_first, other_first = first_class(co, half), first_class(1 - co, half)
    wanted, blocks, at = [], [], 0
    for ref, steps, fresh in zip(e_refs, places, raw):
        e_all[at : at + ref.shape[0], :] = unit_rows(ref[...]) if fresh else ref[...]
        at += ref.shape[0]
        for step, flip in steps:
            z, yl = block_of(step, flip)
            line = lab_ref[pl.ds(z * 4 + yl * 2 + co, 1), :]
            own, other = line - own_first, line - other_first
            in_own = (own >= 0) & (own < half)
            in_other = (other >= 0) & (other < half)
            wanted.append(jnp.where(in_own, own, jnp.where(in_other, other + half, -100)))
            blocks.append(z * 2 + yl)
    wanted = jnp.concatenate(wanted, axis=1) if len(wanted) > 1 else wanted[0]
    place = jnp.broadcast_to(wanted, (8, rows)) - lax.broadcasted_iota(jnp.int32, (8, rows), 0)
    turns = half // chunk

    def product(index, c_ref, s_ref):
        s_ref[...] = lax.dot_general(
            c_ref[pl.ds(index * chunk, chunk), :],
            e_all[...],
            (((1,), (1,)), ((), ())),
            preferred_element_type=f32,
        )

    def finish(total, found, shift):
        found = jnp.max(found, axis=0, keepdims=True)
        here = found > NEVER
        margin = margin_cos(found)
        if shift is None:
            peak, total = total
            top = jnp.max(peak, axis=0, keepdims=True)
            top = jnp.where(here, jnp.maximum(top, margin), top)
            total, shift = total * jnp.exp2((peak - top) * SCALE2), top * SCALE2
        total = jnp.sum(total, axis=0, keepdims=True)
        both = total + jnp.where(here, jnp.exp2(margin * SCALE2 - shift), 0.0)
        log_total = (jnp.log2(both) + shift) * math.log(2.0)
        target = jnp.where(here, logit_scale * margin, 0.0)
        copies = out_ref.shape[0] // 16
        for b, block in enumerate(blocks):
            part = slice(b * 128, (b + 1) * 128)
            line = jnp.concatenate([log_total[:, part], target[:, part]], axis=1)
            spot = pl.multiple_of(block * copies, copies)
            out_ref[pl.ds(spot, copies)] = jnp.broadcast_to(line[None], (copies, 1, 256))
        return total

    def fold(first, s_ref, state):
        sums, found = list(state[:-1]), state[-1]
        here = place - first
        for j in range(chunk // 8):
            cosine = s_ref[j * 8 : (j + 1) * 8, :]
            hit = here == j * 8
            found = jnp.where(hit, cosine, found)
            term = jnp.exp2(jnp.where(hit, NEVER, cosine) * SCALE2 - SHIFT)
            sums[j % len(sums)] = sums[j % len(sums)] + term
        return (*sums, found)

    product(0, own_ref, s_own)

    def body(k, state):
        for turn in range(UNROLL):
            t = k * UNROLL + turn
            product(t, other_ref, s_other)
            state = fold(t * chunk, s_own, state)
            product(jnp.minimum(t + 1, turns - 1), own_ref, s_own)
            state = fold(half + t * chunk, s_other, state)
        return state

    zero, none = jnp.zeros((8, rows), f32), jnp.full((8, rows), 2 * NEVER, f32)
    state = lax.fori_loop(0, turns // UNROLL, body, (zero,) * (1024 // rows) + (none,))
    total = finish(functools.reduce(jnp.add, state[:-1]), state[-1], SHIFT)

    @pl.when(jnp.min(total) < 2.0**-89)
    def _():
        def careful(first, s_ref, state):
            def one(j, state):
                peak, total, found = state
                cosine = s_ref[pl.ds(pl.multiple_of(j * 8, 8), 8), :]
                hit = place == first + j * 8
                found = jnp.where(hit, cosine, found)
                cosine = jnp.where(hit, NEVER, cosine)
                top = jnp.maximum(peak, cosine)
                total = total * jnp.exp2((peak - top) * SCALE2) + jnp.exp2((cosine - top) * SCALE2)
                return top, total, found

            return lax.fori_loop(0, chunk // 8, one, state)

        def again(k, state):
            product(k, own_ref, s_own)
            state = careful(k * chunk, s_own, state)
            product(k, other_ref, s_other)
            return careful(half + k * chunk, s_other, state)

        peak, total, found = lax.fori_loop(0, turns, again, (none * 0.5, zero, none))
        finish((peak, total), found, None)


def stats_call(board, parts, places, own, other, labels, raw=()):
    rows, width = sum(p.shape[0] for p in parts), own.shape[1]
    classes = own.shape[0] + other.shape[0]
    shape = (16 * lax.axis_size("yh") * lax.axis_size("x"), 1, 256)
    chunk = 256
    boards = () if board is None else (board,)
    return pl.pallas_call(
        functools.partial(stats_kernel, tuple(places), raw or (False,) * len(parts), chunk),
        out_shape=jax.ShapeDtypeStruct(shape, f32),
        in_specs=[pl.BlockSpec(memory_space=pltpu.VMEM)] * (3 + len(parts))
        + [pl.BlockSpec(memory_space=pltpu.VMEM)] * len(boards),
        out_specs=pl.BlockSpec(memory_space=pltpu.VMEM),
        scratch_shapes=[
            pltpu.VMEM((rows, width), bf16),
            pltpu.VMEM((chunk, rows), f32),
            pltpu.VMEM((chunk, rows), f32),
        ],
        input_output_aliases={3 + len(parts): 0} if boards else {},
        compiler_params=pltpu.CompilerParams(vmem_limit_bytes=16 * 2**20),
        cost_estimate=pl.CostEstimate(
            flops=2 * rows * classes * width,
            bytes_accessed=classes * width * 2,
            transcendentals=rows * classes,
        ),
    )(labels, own, other, *parts, *boards)


def combine_kernel(got_ref, out_ref):
    n = got_ref.shape[0] // 8
    even = lax.rem(lax.broadcasted_iota(jnp.int32, (8, 128), 0), 2) == 0
    tiles = [got_ref[i * 8 : (i + 1) * 8, :] for i in range(n)]
    peak = functools.reduce(jnp.maximum, tiles)
    peak = jnp.max(jnp.where(even, peak, -2.0 * logit_scale), axis=0, keepdims=True)
    sums = [jnp.zeros((8, 128), f32)] * 4
    for i, tile in enumerate(tiles):
        fall = jnp.where(even, (tile - peak) * math.log2(math.e), -1000.0)
        sums[i % 4] = sums[i % 4] + jnp.exp2(fall)
    total = jnp.sum(functools.reduce(jnp.add, sums), axis=0, keepdims=True)
    target = functools.reduce(jnp.add, tiles)
    target = jnp.sum(jnp.where(even, 0.0, target), axis=0, keepdims=True)
    out_ref[...] = peak + jnp.log(total) - target


def combine_call(got):
    return pl.pallas_call(
        combine_kernel,
        out_shape=jax.ShapeDtypeStruct((1, 128), f32),
        in_specs=[pl.BlockSpec(memory_space=pltpu.VMEM)],
        out_specs=pl.BlockSpec(memory_space=pltpu.VMEM),
        compiler_params=pltpu.CompilerParams(vmem_limit_bytes=2**20),
        name="combine",
    )(got)


def moved(value, axis, by):
    n = lax.axis_size(axis)
    return lax.ppermute(value, axis, [(i, (i + by) % n) for i in range(n)])


def to_lower(value):
    spots = [(yl, yh) for yl in range(2) for yh in range(2)]
    pairs = []
    for yl, yh in spots:
        y = (yh * 2 + yl + (1 if yl else -1)) % 4
        pairs.append((spots.index((yl, yh)), spots.index((y % 2, y // 2))))
    return lax.ppermute(value, ("yl", "yh"), pairs)


def shards(embeddings, centers, labels):
    fence = lax.optimization_barrier
    up1 = moved(embeddings, "z", 1)
    down1 = moved(embeddings, "z", -1)
    lines = labels.reshape(-1, 128)
    own = unit_centers(centers)
    other = moved(own, "co", 1)

    up1, down1, own = fence((up1, down1, own))
    up2 = moved(up1, "z", 1)
    down2 = moved(down1, "z", -1)
    pair1 = unit_call(up1, down1)
    side1 = moved(pair1, "yl", 1)
    late, side_seen = fence((embeddings, pair1))
    beside = to_lower(late)
    board = stats_call(None, [side_seen], [[(-1, 0), (1, 0)]], own, other, lines)

    up2, down2, board = fence((up2, down2, board))
    up3 = moved(up2, "z", 1)
    down3 = moved(down2, "z", -1)
    pair2 = unit_call(up2, down2)
    side2 = moved(pair2, "yl", 1)
    board = stats_call(
        board,
        [embeddings, beside, side1],
        [[(0, 0)], [(0, 1)], [(-1, 1), (1, 1)]],
        own,
        other,
        lines,
        raw=(True, True, False),
    )

    up3, down3, board = fence((up3, down3, board))
    far = moved(up3, "z", 1)
    pair3 = unit_call(up3, down3)
    side3 = to_lower(pair3)
    board = stats_call(
        board, [pair2, pair3], [[(-2, 0), (2, 0)], [(-3, 0), (3, 0)]], own, other, lines
    )
    far, board = fence((far, board))
    far_side = moved(far, "yl", 1)
    side2, board = fence((side2, board))
    board = stats_call(board, [side2], [[(-2, 1), (2, 1)]], own, other, lines)
    side3, board = fence((side3, board))
    board = stats_call(board, [side3], [[(-3, 1), (3, 1)]], own, other, lines)
    far_side, board = fence((far_side, board))
    board = stats_call(board, [far, far_side], [[(4, 0)], [(4, 1)]], own, other, lines, raw=(True, True))

    got = lax.all_to_all(board, SAME_CORE, split_axis=0, concat_axis=0, tiled=True)
    return combine_call(got.reshape(-1, 128)).reshape(-1)


def solution(mesh):
    split = Mesh(mesh.devices.reshape(8, 2, 2, 2, 4), AXES)
    return jax.shard_map(
        shards,
        mesh=split,
        in_specs=(P(ROW, None), P(AXES, None), P()),
        out_specs=P(ROW),
        check_vma=False,
    )
```
